32 devices in a mesh: seq: 8 (over z, y), tp: 4 (over x, core).
Axes of the slice: x: 2, y: 2, z: 4, core: 2. Of those that a mesh axis runs over, the one named last changes fastest.
Arguments:
- queries: bfloat16 [1, 2048, 4096], P(None, 'seq', 'tp'), may hold values from -13 to 13
- key_rows: bfloat16 [1, 2048, 2048], P(None, 'seq', 'tp'), may hold values from -13 to 13
- value_rows: bfloat16 [1, 2048, 2048], P(None, 'seq', 'tp'), may hold values from -6 to 6
- residual: bfloat16 [1, 2048, 3584], P(None, 'seq', 'tp'), may hold values from -6 to 6
- out_weight: bfloat16 [4096, 3584], P('tp')
- post_scale: float32 [3584], P('tp'), may hold values from 0.1 to 1.9
- lengths: int32 [1], replicated, may hold values from 512 to 2047
- owners: int32 [1, 8], replicated, may hold values from 0 to 7, each once within a row
Outputs:
- hidden_out: bfloat16 [1, 2048, 3584], P(None, 'seq', 'tp')
- cache_keys: bfloat16 [1, 4096, 2048], P(None, 'seq', 'tp')
- cache_values: bfloat16 [1, 4096, 2048], P(None, 'seq', 'tp')
The draws below stay inside these ranges and needn't reach their ends.
Inputs may be any that keep to these rules, and one draw needn't show every extreme that they name: Each row of owners names every number from 0 to 7 once.
All inputs are finite; a program needn't handle non-finite values.
Results may differ from the reference program's by a relative error of at most 0.0083.
Values may be sent and summed in bfloat16 or wider, within the bound.
A program may use at most 64 MiB of HBM per device.

```python
import jax
import jax.numpy as jnp
from jax import lax

D = 3584
QH = 16
KVH = 8
HD = 256
WINDOW = 4096
SEQS = 1
SHARD = 256
LENGTH = 2048
N_SEQ = 8


def draw_out_weight(key, part):
    entry_key, jitter_key = jax.random.split(jax.random.fold_in(key, 17))
    fan_in = QH * HD
    entries = jax.random.normal(entry_key, (fan_in, D), jnp.float32)
    rising = jnp.exp(jnp.linspace(jnp.log(0.5), jnp.log(5.0), D)).astype(jnp.float32)
    jitter = jnp.exp(jax.random.uniform(jitter_key, (D,), jnp.float32, -0.35, 0.35))
    return (entries * (rising * jitter)[None, :] * fan_in ** (-0.5)).astype(jnp.bfloat16)


def planted_lift(key):
    mask_key, scale_key, sign_key = jax.random.split(jax.random.fold_in(key, 29), 3)
    fraction = 0.03
    chosen = jax.random.bernoulli(mask_key, fraction, (SEQS, LENGTH))
    amplitude = jax.random.uniform(scale_key, (SEQS, LENGTH), jnp.float32, 8.0, 13.5) * HD ** 0.25
    raised = jnp.where(chosen, amplitude, jnp.zeros_like(amplitude))
    directions = jax.random.rademacher(sign_key, (KVH, HD), jnp.float32) * HD ** (-0.5)
    return (raised, directions)


def background_rows(noise_key, width):
    background = jnp.clip(jax.random.normal(noise_key, (SEQS, LENGTH, width), jnp.float32), -6.0, 6.0)
    return background


def draw_queries(key, part):
    raised, directions = planted_lift(key)
    background = background_rows(jax.random.fold_in(key, 31), QH * HD)
    repeated = jnp.repeat(directions, QH // KVH, axis=0).reshape(QH * HD)
    return (background + raised[:, :, None] * repeated[None, None, :]).astype(jnp.bfloat16)


def draw_key_rows(key, part):
    raised, directions = planted_lift(key)
    background = background_rows(jax.random.fold_in(key, 37), KVH * HD)
    flattened = directions.reshape(KVH * HD)
    return (background + raised[:, :, None] * flattened[None, None, :]).astype(jnp.bfloat16)


def shard_levels(stream_key, dims, shards, smallest, high):
    def one(dim, parts):
        heights = jax.random.uniform(jax.random.fold_in(jax.random.fold_in(stream_key, 6), dim), (parts,), jnp.float32, smallest / len(shards), high / len(shards))
        return jnp.repeat(jnp.exp(heights), dims[dim] // parts).reshape((-1,) + (1,) * (len(dims) - dim - 1))

    loudness = one(*shards[0])
    for cut in shards[1:]:
        loudness = loudness * one(*cut)
    return loudness


def scatter_about(own_key, extent, scale, most, pieces=(), kind=jnp.bfloat16):
    loudness = shard_levels(own_key, extent, pieces, -0.22, 0.18) if pieces else 1.0
    values = jax.random.normal(own_key, extent, jnp.float32) * scale * loudness
    return jnp.minimum(jnp.maximum(values, -most), most).astype(kind)


def setup_inputs(seed: int = 0) -> dict:
    keys = jax.random.split(jax.random.key(seed), 9)
    queries = draw_queries(jax.random.fold_in(keys[8], 71), 0)
    key_rows = draw_key_rows(jax.random.fold_in(keys[8], 71), 0)
    value_rows = scatter_about(keys[2], (SEQS, LENGTH, KVH * HD), 1.0, 6.0, ((1, 8), (2, 4)))
    residual = scatter_about(keys[3], (SEQS, LENGTH, D), 1.0, 6.0, ((1, 8), (2, 4)))
    out_weight = draw_out_weight(jax.random.fold_in(keys[8], 71), 0)
    post_scale = jnp.clip(1.0 + 0.18 * jax.random.normal(keys[5], (D,), jnp.float32), 0.1, 1.9)
    lengths = jax.random.randint(keys[6], (SEQS,), min(WINDOW, LENGTH) // 4, min(WINDOW, LENGTH)).astype(jnp.int32)
    owners = jax.vmap(lambda own: jax.random.permutation(own, N_SEQ))(jax.random.split(keys[7], SEQS)).reshape((SEQS, N_SEQ)).astype(jnp.int32)
    return {"queries": queries, "key_rows": key_rows, "value_rows": value_rows, "residual": residual, "out_weight": out_weight, "post_scale": post_scale, "lengths": lengths, "owners": owners}


soft_cap = 50.0
norm_eps = 1e-06

def attend_rows(queries, padded_keys, padded_values, row_start):
    group_size = QH // KVH
    query_block = lax.dynamic_slice_in_dim(queries, row_start, SHARD, 1).astype(jnp.float32).reshape(SEQS, SHARD, KVH, group_size, HD)
    key_block = lax.dynamic_slice_in_dim(padded_keys, row_start, WINDOW + SHARD, 1).astype(jnp.float32).reshape(SEQS, WINDOW + SHARD, KVH, HD)
    value_block = lax.dynamic_slice_in_dim(padded_values, row_start, WINDOW + SHARD, 1).astype(jnp.float32).reshape(SEQS, WINDOW + SHARD, KVH, HD)
    scores = jnp.einsum('sqhgd,skhd->shgqk', query_block, key_block) * HD ** (-0.5)
    capped = soft_cap * jnp.tanh(scores / soft_cap)
    query_pos = row_start + jnp.arange(SHARD, dtype=jnp.int32)
    key_pos = row_start - WINDOW + jnp.arange(WINDOW + SHARD, dtype=jnp.int32)
    spread = query_pos[:, None] - key_pos[None, :]
    live_mask = (spread >= 0) & (spread < WINDOW) & (key_pos[None, :] >= 0)
    weights = jnp.where(live_mask, jnp.exp(capped), jnp.zeros_like(capped))
    totals = lax.optimization_barrier(jnp.sum(weights, axis=-1))
    rounded = lax.optimization_barrier(weights.astype(jnp.bfloat16)).astype(jnp.float32)
    mixture = jnp.einsum('shgqk,skhd->sqhgd', rounded, value_block)
    attended = mixture / jnp.transpose(totals, (0, 3, 1, 2))[..., None]
    return attended.astype(jnp.bfloat16).reshape(SEQS, SHARD, QH * HD)

def window_rows(rows_in, length):
    slots = jnp.arange(WINDOW, dtype=jnp.int32)
    anchor = length - WINDOW + jnp.mod(slots - length + WINDOW, WINDOW)
    taken = jnp.take(rows_in, jnp.clip(anchor, 0, LENGTH - 1), axis=0)
    return jnp.where((anchor >= 0)[:, None], taken, jnp.zeros_like(taken))

def owner_layout(slotted, owner_row):
    devices = jnp.arange(N_SEQ, dtype=jnp.int32)
    matches = owner_row[:, None] == devices[None, :]
    inverse = lax.optimization_barrier(jnp.sum(jnp.where(matches, devices[:, None], jnp.zeros_like(devices)[:, None]), axis=0))
    local = jnp.arange(WINDOW // N_SEQ, dtype=jnp.int32)
    block_rows = SHARD // N_SEQ
    chosen = local[None, :] // block_rows * SHARD + inverse[:, None] * block_rows + local[None, :] % block_rows
    return jnp.take(slotted, chosen.reshape(-1), axis=0)

def reference(queries, key_rows, value_rows, residual, out_weight, post_scale, lengths, owners):
    front = jnp.zeros((SEQS, WINDOW, KVH * HD), key_rows.dtype)
    padded_keys = jnp.concatenate([front, key_rows], axis=1)
    padded_values = jnp.concatenate([front, value_rows], axis=1)
    starts = jnp.arange(LENGTH // SHARD, dtype=jnp.int32) * SHARD
    blocks = lax.map(lambda row_start: attend_rows(queries, padded_keys, padded_values, row_start), starts)
    attended = jnp.transpose(blocks, (1, 0, 2, 3)).reshape(SEQS * LENGTH, QH * HD)
    branch = jnp.dot(attended, out_weight, preferred_element_type=jnp.float32)
    mean_square = lax.optimization_barrier(jnp.mean(branch * branch, axis=-1, keepdims=True))
    normed = branch * lax.rsqrt(mean_square + norm_eps) * post_scale
    hidden_out = (residual.reshape(SEQS * LENGTH, D).astype(jnp.float32) + normed).astype(jnp.bfloat16).reshape(SEQS, LENGTH, D)
    cache_keys = jnp.stack([owner_layout(window_rows(key_rows[seq_index], lengths[seq_index]), owners[seq_index]) for seq_index in range(SEQS)])
    cache_values = jnp.stack([owner_layout(window_rows(value_rows[seq_index], lengths[seq_index]), owners[seq_index]) for seq_index in range(SEQS)])
    return (hidden_out, cache_keys, cache_values)
```

```python
import functools

import jax
import jax.numpy as jnp
from jax import lax
from jax.experimental import pallas as pl
from jax.experimental.pallas import tpu as pltpu
from jax.sharding import PartitionSpec as P

D = 3584
HD = 256
WINDOW = 4096
MESH = pl.DeviceIdType.MESH
LOG2E = 1.4426950408889634
ROWS = 128


soft_cap = 50.0
norm_eps = 1e-06


def shifted(x, axis, by):
    peers = lax.axis_size(axis)
    pairs = [(i, i + by) for i in range(peers) if 0 <= i + by < peers]
    return lax.ppermute(x, axis, pairs)


def attend_block(grouped, block_keys, block_values, query_pos, key_pos, state_pair):
    numerator, denominator = state_pair
    seq_count, query_count, kv_local, group_size, head_size = grouped.shape
    keyed_rows = block_keys.reshape(seq_count, block_keys.shape[1], kv_local, head_size)
    valued_rows = block_values.reshape(seq_count, block_values.shape[1], kv_local, head_size)
    scores = jnp.einsum(
        "sqhgd,skhd->shgqk", grouped, keyed_rows, preferred_element_type=jnp.float32
    ) * head_size ** (-0.5)
    capped = soft_cap * jnp.tanh(scores / soft_cap)
    spread = query_pos[:, None] - key_pos[None, :]
    live_mask = (spread >= 0) & (spread < WINDOW) & (key_pos[None, :] >= 0)
    weights = jnp.where(live_mask, jnp.exp(capped), jnp.zeros_like(capped))
    denominator = denominator + jnp.sum(weights, axis=-1)
    numerator = numerator + jnp.einsum(
        "shgqk,skhd->sqhgd",
        weights.astype(jnp.bfloat16),
        valued_rows,
        preferred_element_type=jnp.float32,
    )
    return (numerator, denominator)


def reorder_blocks(blocked, ordering):
    return blocked[ordering]


def local(queries, key_rows, value_rows, residual, out_weight, post_scale, lengths, owners):
    seq_count, shard_len, query_width = queries.shape
    seq_size = lax.axis_size("seq")
    if (
        seq_count == 1 and lax.axis_size("tp") == 4 and seq_size % 2 == 0
        and seq_size * shard_len <= WINDOW
    ):
        return fused(
            seq_size, queries, key_rows, value_rows, residual, out_weight, post_scale, lengths,
            owners,
        )
    kv_width = key_rows.shape[2]
    kv_local = kv_width // HD
    group_size = query_width // kv_width
    grouped = queries.reshape(seq_count, shard_len, kv_local, group_size, HD)
    position = lax.axis_index("seq")
    seq_devices = lax.axis_size("seq")
    offsets = jnp.arange(shard_len, dtype=jnp.int32)
    query_pos = position * shard_len + offsets
    numerator = jnp.zeros((seq_count, shard_len, kv_local, group_size, HD), jnp.float32)
    denominator = jnp.zeros((seq_count, kv_local, group_size, shard_len), jnp.float32)
    state_pair = attend_block(
        grouped, key_rows, value_rows, query_pos, query_pos, (numerator, denominator)
    )
    hop_count = min(WINDOW // shard_len, seq_devices - 1)
    arrived = []
    current = (key_rows, value_rows)
    for hop_index in range(1, hop_count + 1):
        current = shifted((current[0], current[1]), "seq", 1)
        arrived.append((hop_index, current))
        if len(arrived) == 2 or hop_index == hop_count:
            ordered = arrived[::-1]
            block_keys = jnp.concatenate([member[1][0] for member in ordered], axis=1)
            block_values = jnp.concatenate([member[1][1] for member in ordered], axis=1)
            block_pos = jnp.concatenate(
                [(position - member[0]) * shard_len + offsets for member in ordered]
            )
            state_pair = attend_block(
                grouped, block_keys, block_values, query_pos, block_pos, state_pair
            )
            arrived = []
    numerator, denominator = state_pair
    attended = (numerator / jnp.transpose(denominator, (0, 3, 1, 2))[..., None]).astype(
        jnp.bfloat16
    )
    partial_value = jnp.dot(
        attended.reshape(seq_count * shard_len, query_width),
        out_weight,
        preferred_element_type=jnp.float32,
    )
    partial_value = partial_value.reshape(seq_count, shard_len, out_weight.shape[1])
    branch = lax.psum_scatter(partial_value, "tp", scatter_dimension=2, tiled=True)
    squares = lax.psum(jnp.sum(branch * branch, axis=-1), "tp")
    normed = branch * lax.rsqrt(squares / D + norm_eps)[..., None] * post_scale
    hidden_out = (residual.astype(jnp.float32) + normed).astype(jnp.bfloat16)
    block_rows = shard_len // seq_devices
    slot_span = WINDOW // shard_len
    live_rows = (query_pos[None, :] >= lengths[:, None] - WINDOW) & (
        query_pos[None, :] < lengths[:, None]
    )
    kept_keys = jnp.where(live_rows[..., None], key_rows, jnp.zeros_like(key_rows))
    kept_values = jnp.where(live_rows[..., None], value_rows, jnp.zeros_like(value_rows))
    devices = jnp.arange(seq_devices, dtype=jnp.int32)
    matches = owners[:, :, None] == devices[None, None, :]
    inverse = jnp.sum(
        jnp.where(matches, devices[None, :, None], jnp.zeros_like(devices)[None, :, None]), axis=1
    )
    outgoing_keys = jax.vmap(reorder_blocks)(
        kept_keys.reshape(seq_count, seq_devices, block_rows, kv_width), inverse
    )
    outgoing_values = jax.vmap(reorder_blocks)(
        kept_values.reshape(seq_count, seq_devices, block_rows, kv_width), inverse
    )
    incoming = (
        lax.all_to_all(outgoing_keys, "seq", split_axis=1, concat_axis=1, tiled=True),
        lax.all_to_all(outgoing_values, "seq", split_axis=1, concat_axis=1, tiled=True),
    )
    selector = (
        devices[None, :] % slot_span == jnp.arange(slot_span, dtype=jnp.int32)[:, None]
    ).astype(jnp.bfloat16)
    cache_keys = (
        jnp.einsum("md,sdbf->smbf", selector, incoming[0], preferred_element_type=jnp.float32)
        .astype(jnp.bfloat16)
        .reshape(seq_count, slot_span * block_rows, kv_width)
    )
    cache_values = (
        jnp.einsum("md,sdbf->smbf", selector, incoming[1], preferred_element_type=jnp.float32)
        .astype(jnp.bfloat16)
        .reshape(seq_count, slot_span * block_rows, kv_width)
    )
    return (hidden_out, cache_keys, cache_values)


def layer_kernel(
    n, q_ref, k_ref, v_ref, res_ref, scale_ref, len_ref, own_ref, w_ref,
    hid_ref, ck_ref, cv_ref,
    kbuf, vbuf, wbuf, acc, den, att, to_sib, to_x, to_sib2, from_sib, from_x, from_sib2,
    total, sq_out, sq_in,
    send_sem, recv_sem, w_sem, rs_send, rs_recv, sq_send, sq_recv,
):
    nz = n // 2
    me = lax.axis_index("seq")
    t = lax.axis_index("tp")
    z, y = me // 2, me % 2
    x, c = t // 2, t % 2
    sib = x * 2 + (1 - c)
    across = (1 - x) * 2 + c
    diagonal = (1 - x) * 2 + (1 - c)
    shard = q_ref.shape[0]
    heads = q_ref.shape[1] // HD
    group = q_ref.shape[1] // k_ref.shape[1]
    bufs = (kbuf, vbuf)
    own = (k_ref, v_ref)

    def w_copy(f):
        return pltpu.make_async_copy(
            w_ref.at[:, pl.ds(f * res_ref.shape[1], res_ref.shape[1])], wbuf.at[f], w_sem.at[f]
        )

    partner = z * 2 + (1 - y)
    barrier = pltpu.get_barrier_semaphore()
    for peer in (sib, across, diagonal):
        pl.semaphore_signal(barrier, inc=1, device_id={"tp": peer}, device_id_type=MESH)
    pl.semaphore_signal(barrier, inc=1, device_id={"seq": partner}, device_id_type=MESH)

    @pl.when(z < nz - 1)
    def _():
        pl.semaphore_signal(barrier, inc=1, device_id={"seq": me + 2}, device_id_type=MESH)

    @pl.when(z > 0)
    def _():
        pl.semaphore_signal(barrier, inc=1, device_id={"seq": me - 2}, device_id_type=MESH)

    @pl.when((z > 0) & (z < nz - 1))
    def _():
        pl.semaphore_wait(barrier, 6)

    @pl.when((z == 0) | (z == nz - 1))
    def _():
        pl.semaphore_wait(barrier, 5)

    def routes(zo, yo, h, mine=False):
        special = ((zo == 0) | (zo == nz - 1)) if h == 1 else False
        line = (yo == y) | special
        crossing = (yo == y) & ((zo == z) | jnp.logical_not(special))
        origin = zo * 2 + yo
        plan = (
            (line & (zo <= z) & (z < nz - 1), me + 2),
            (line & (zo >= z) & (z > 0), me - 2),
            (crossing, partner),
        )
        out = []
        for way, (go, to) in enumerate(plan):
            copy = pltpu.make_async_remote_copy(
                src_ref=own[h] if mine else bufs[h].at[origin],
                dst_ref=bufs[h].at[origin],
                send_sem=send_sem.at[origin, h, way],
                recv_sem=recv_sem.at[origin, h],
                device_id={"seq": to},
                device_id_type=MESH,
            )
            out.append((go, copy))
        return out

    def start(zo, yo, h, mine=False):
        for go, copy in routes(zo, yo, h, mine):
            pl.when(go)(copy.start)

    def handle(zo, yo, h):
        routes(zo, yo, h)[0][1].wait_recv()
        start(zo, yo, h)

    start(z, y, 0, True)
    start(z, y, 1, True)
    for f in range(4):
        w_copy(f).start()

    def attend(keys, values, masked):
        for h in range(heads):
            cols = pl.ds((h // group) * HD, HD)
            s = lax.dot_general(
                q_ref[:, h * HD : (h + 1) * HD], keys[:, cols], (((1,), (1,)), ((), ())),
                preferred_element_type=jnp.float32,
            )
            w = jnp.exp2(jnp.tanh(s * (HD ** (-0.5) / soft_cap)) * (soft_cap * LOG2E))
            if masked:
                keep = lax.broadcasted_iota(jnp.int32, w.shape, 0) >= lax.broadcasted_iota(
                    jnp.int32, w.shape, 1
                )
                w = jnp.where(keep, w, 0.0)
            folded = w[:, :128]
            for i in range(1, w.shape[1] // 128):
                folded = folded + w[:, i * 128 : (i + 1) * 128]
            o = jnp.dot(w.astype(jnp.bfloat16), values[:, cols], preferred_element_type=jnp.float32)
            if masked:
                den[h] = folded
                acc[h] = o
            else:
                den[h] += folded
                acc[h] += o

    attend(k_ref, v_ref, True)

    def phase(d, carry):
        e = d - 1
        for h in (0, 1):
            for sign in (-1, 1):
                zz = z + sign * d
                pl.when((zz >= 0) & (zz < nz))(functools.partial(handle, zz, y, h))
        for h in (1, 0):
            for sign in (-1, 1):
                zz = z + sign * e
                there = (zz >= 0) & (zz < nz)
                if sign == 1:
                    there = there & (e > 0)
                pl.when(there)(functools.partial(handle, zz, 1 - y, h))

        def one(i, carry):
            zz = z - d + i
            origin = zz * 2 + jnp.where(i == 0, y, 1 - y)

            @pl.when((zz >= 0) & (origin < me))
            def _():
                attend(kbuf.at[origin], vbuf.at[origin], False)

            return carry

        lax.fori_loop(0, 2, one, 0)
        return carry

    lax.fori_loop(1, nz + 1, phase, 0)

    for h in range(heads):
        att[:, h * HD : (h + 1) * HD] = (
            acc[h] / jnp.sum(den[h], axis=-1, keepdims=True)
        ).astype(jnp.bfloat16)

    chunks = shard // ROWS

    def rs_copy(kind, r, src, dst, to):
        return pltpu.make_async_remote_copy(
            src_ref=src.at[r], dst_ref=dst.at[r], send_sem=rs_send.at[kind, r],
            recv_sem=rs_recv.at[kind, r], device_id={"tp": to}, device_id_type=MESH,
        )

    def sib_copy(r):
        return rs_copy(0, r, to_sib, from_sib, sib)

    def x_copy(r):
        return rs_copy(1, r, to_x, from_x, across)

    def sib2_copy(r):
        return rs_copy(2, r, to_sib2, from_sib2, sib)

    def part(f, r):
        rows = att[pl.ds(pl.multiple_of(r * ROWS, ROWS), ROWS), :]
        return jnp.dot(rows, wbuf[f], preferred_element_type=jnp.float32)

    for f in range(4):
        w_copy(f).wait()

    def first(r, carry):
        to_sib[r] = part(diagonal, r).astype(jnp.bfloat16)
        sib_copy(r).start()
        return carry

    def second(r, carry):
        mine = part(across, r)
        sib_copy(r).wait_recv()
        to_x[r] = (mine + from_sib[r].astype(jnp.float32)).astype(jnp.bfloat16)
        x_copy(r).start()
        return carry

    def third(r, carry):
        to_sib2[r] = part(sib, r).astype(jnp.bfloat16)
        sib2_copy(r).start()
        return carry

    def fourth(r, carry):
        total[r] = part(t, r)
        return carry

    for step in (first, second, third, fourth):
        lax.fori_loop(0, chunks, step, 0)

    block_rows = shard // n
    block = own_ref[0, 0] * 0
    for b in range(n):
        block = block + jnp.where(own_ref[0, b] == me, b, 0)
    kbuf[me] = k_ref[...]
    vbuf[me] = v_ref[...]
    length = len_ref[0]
    local_row = lax.broadcasted_iota(jnp.int32, (block_rows, k_ref.shape[1]), 0)
    chosen = jnp.full(local_row.shape, block, jnp.int32)
    bound = jnp.full(local_row.shape, length, jnp.int32)

    def cache(origin, carry):
        pos = local_row + chosen * block_rows + origin * shard
        live = (pos < bound) & (pos >= bound - WINDOW)
        spot = jnp.where(live, chosen, -1)
        for buf, out in ((kbuf, ck_ref), (vbuf, cv_ref)):
            got = jnp.zeros(local_row.shape, jnp.float32)
            for b in range(n):
                rows = buf[origin, b * block_rows : (b + 1) * block_rows, :]
                got = jnp.where(spot == b, rows.astype(jnp.float32), got)
            start_row = pl.multiple_of(origin * block_rows, block_rows)
            out[pl.ds(start_row, block_rows), :] = got.astype(jnp.bfloat16)
        return carry

    lax.fori_loop(0, n, cache, 0)
    rest = ck_ref.shape[0] - n * block_rows
    if rest:
        for out in (ck_ref, cv_ref):
            out[n * block_rows :, :] = jnp.zeros((rest, k_ref.shape[1]), jnp.bfloat16)

    for r in range(chunks):
        sib2_copy(r).wait_recv()
        x_copy(r).wait_recv()
        branch = total[r] + from_sib2[r].astype(jnp.float32) + from_x[r].astype(jnp.float32)
        total[r] = branch
        squared = branch * branch
        folded = squared[:, :128]
        for i in range(1, squared.shape[1] // 128):
            folded = folded + squared[:, i * 128 : (i + 1) * 128]
        line = jnp.sum(folded.T, axis=0, keepdims=True)
        sq_out[:, r * ROWS : (r + 1) * ROWS] = jnp.broadcast_to(line, (8, ROWS))

    def sq_copy(i, to, slot):
        return pltpu.make_async_remote_copy(
            src_ref=sq_out, dst_ref=sq_in.at[slot], send_sem=sq_send.at[i],
            recv_sem=sq_recv.at[slot], device_id={"tp": to}, device_id_type=MESH,
        )

    peers = (sib, across, diagonal)
    for i, peer in enumerate(peers):
        sq_copy(i, peer, t).start()
    squares = sq_out[...]
    for i, peer in enumerate(peers):
        sq_copy(i, peer, peer).wait_recv()
        squares = squares + sq_in[peer]
    factor = lax.rsqrt(squares / D + norm_eps)
    for r in range(chunks):
        line = jnp.broadcast_to(factor[:1, r * ROWS : (r + 1) * ROWS], (128, ROWS))
        spread = line.T
        for i in range(res_ref.shape[1] // 128):
            cols = slice(i * 128, (i + 1) * 128)
            rows = slice(r * ROWS, (r + 1) * ROWS)
            normed = total[r, :, cols] * spread * scale_ref[:, cols]
            hid_ref[rows, cols] = (res_ref[rows, cols].astype(jnp.float32) + normed).astype(
                jnp.bfloat16
            )

    for i, peer in enumerate(peers):
        sq_copy(i, peer, t).wait_send()
    for r in range(chunks):
        sib_copy(r).wait_send()
        x_copy(r).wait_send()
        sib2_copy(r).wait_send()
    for h in (0, 1):
        for go, copy in routes(z, y, h, True):
            pl.when(go)(copy.wait_send)

    def drain(origin, carry):
        @pl.when(origin != me)
        def _():
            for h in (0, 1):
                for go, copy in routes(origin // 2, origin % 2, h):
                    pl.when(go)(copy.wait_send)

        return carry

    lax.fori_loop(0, n, drain, 0)


def fused(n, queries, key_rows, value_rows, residual, out_weight, post_scale, lengths, owners):
    shard, q_width = queries.shape[1:]
    kv_width = key_rows.shape[2]
    width = residual.shape[2]
    heads = q_width // HD
    chunks = shard // ROWS
    cache_rows = WINDOW // n
    vmem = pl.BlockSpec(memory_space=pltpu.VMEM)
    smem = pl.BlockSpec(memory_space=pltpu.SMEM)
    half = pltpu.VMEM((chunks, ROWS, width), jnp.bfloat16)
    hidden, ck, cv = pl.pallas_call(
        functools.partial(layer_kernel, n),
        out_shape=(
            jax.ShapeDtypeStruct((shard, width), jnp.bfloat16),
            jax.ShapeDtypeStruct((cache_rows, kv_width), jnp.bfloat16),
            jax.ShapeDtypeStruct((cache_rows, kv_width), jnp.bfloat16),
        ),
        in_specs=[vmem] * 5 + [smem] * 2 + [pl.BlockSpec(memory_space=pl.ANY)],
        out_specs=(vmem,) * 3,
        scratch_shapes=[
            pltpu.VMEM((n, shard, kv_width), jnp.bfloat16),
            pltpu.VMEM((n, shard, kv_width), jnp.bfloat16),
            pltpu.VMEM((4, q_width, width), jnp.bfloat16),
            pltpu.VMEM((heads, shard, HD), jnp.float32),
            pltpu.VMEM((heads, shard, 128), jnp.float32),
            pltpu.VMEM((shard, q_width), jnp.bfloat16),
            half, half, half, half, half, half,
            pltpu.VMEM((chunks, ROWS, width), jnp.float32),
            pltpu.VMEM((8, shard), jnp.float32),
            pltpu.VMEM((4, 8, shard), jnp.float32),
            pltpu.SemaphoreType.DMA((n, 2, 3)),
            pltpu.SemaphoreType.DMA((n, 2)),
            pltpu.SemaphoreType.DMA((4,)),
            pltpu.SemaphoreType.DMA((3, chunks)),
            pltpu.SemaphoreType.DMA((3, chunks)),
            pltpu.SemaphoreType.DMA((3,)),
            pltpu.SemaphoreType.DMA((4,)),
        ],
        compiler_params=pltpu.CompilerParams(
            collective_id=0, has_side_effects=True, vmem_limit_bytes=48 * 1024 * 1024
        ),
    )(
        queries[0], key_rows[0], value_rows[0], residual[0], post_scale[None], lengths, owners,
        out_weight,
    )
    return hidden[None], ck[None], cv[None]


def solution(mesh):
    placed = (
        P(None, "seq", "tp"),
        P(None, "seq", "tp"),
        P(None, "seq", "tp"),
        P(None, "seq", "tp"),
        P("tp", None),
        P("tp"),
        P(),
        P(),
    )
    return jax.shard_map(
        local,
        mesh=mesh,
        in_specs=placed,
        out_specs=(P(None, "seq", "tp"), P(None, "seq", "tp"), P(None, "seq", "tp")),
        check_vma=False,
    )
```

```python
import functools

import jax
import jax.numpy as jnp
from jax import lax
from jax.experimental import pallas as pl
from jax.experimental.pallas import tpu as pltpu
from jax.sharding import PartitionSpec as P

D = 3584
HD = 256
WINDOW = 4096
MESH = pl.DeviceIdType.MESH
LOG2E = 1.4426950408889634
ROWS = 128


soft_cap = 50.0
norm_eps = 1e-06


def shifted(x, axis, by):
    peers = lax.axis_size(axis)
    pairs = [(i, i + by) for i in range(peers) if 0 <= i + by < peers]
    return lax.ppermute(x, axis, pairs)


def attend_block(grouped, block_keys, block_values, query_pos, key_pos, state_pair):
    numerator, denominator = state_pair
    seq_count, query_count, kv_local, group_size, head_size = grouped.shape
    keyed_rows = block_keys.reshape(seq_count, block_keys.shape[1], kv_local, head_size)
    valued_rows = block_values.reshape(seq_count, block_values.shape[1], kv_local, head_size)
    scores = jnp.einsum(
        "sqhgd,skhd->shgqk", grouped, keyed_rows, preferred_element_type=jnp.float32
    ) * head_size ** (-0.5)
    capped = soft_cap * jnp.tanh(scores / soft_cap)
    spread = query_pos[:, None] - key_pos[None, :]
    live_mask = (spread >= 0) & (spread < WINDOW) & (key_pos[None, :] >= 0)
    weights = jnp.where(live_mask, jnp.exp(capped), jnp.zeros_like(capped))
    denominator = denominator + jnp.sum(weights, axis=-1)
    numerator = numerator + jnp.einsum(
        "shgqk,skhd->sqhgd",
        weights.astype(jnp.bfloat16),
        valued_rows,
        preferred_element_type=jnp.float32,
    )
    return (numerator, denominator)


def reorder_blocks(blocked, ordering):
    return blocked[ordering]


def local(queries, key_rows, value_rows, residual, out_weight, post_scale, lengths, owners):
    seq_count, shard_len, query_width = queries.shape
    seq_size = lax.axis_size("seq")
    if (
        seq_count == 1 and lax.axis_size("tp") == 4 and seq_size % 2 == 0
        and seq_size * shard_len <= WINDOW
    ):
        return fused(
            seq_size, queries, key_rows, value_rows, residual, out_weight, post_scale, lengths,
            owners,
        )
    kv_width = key_rows.shape[2]
    kv_local = kv_width // HD
    group_size = query_width // kv_width
    grouped = queries.reshape(seq_count, shard_len, kv_local, group_size, HD)
    position = lax.axis_index("seq")
    seq_devices = lax.axis_size("seq")
    offsets = jnp.arange(shard_len, dtype=jnp.int32)
    query_pos = position * shard_len + offsets
    numerator = jnp.zeros((seq_count, shard_len, kv_local, group_size, HD), jnp.float32)
    denominator = jnp.zeros((seq_count, kv_local, group_size, shard_len), jnp.float32)
    state_pair = attend_block(
        grouped, key_rows, value_rows, query_pos, query_pos, (numerator, denominator)
    )
    hop_count = min(WINDOW // shard_len, seq_devices - 1)
    arrived = []
    current = (key_rows, value_rows)
    for hop_index in range(1, hop_count + 1):
        current = shifted((current[0], current[1]), "seq", 1)
        arrived.append((hop_index, current))
        if len(arrived) == 2 or hop_index == hop_count:
            ordered = arrived[::-1]
            block_keys = jnp.concatenate([member[1][0] for member in ordered], axis=1)
            block_values = jnp.concatenate([member[1][1] for member in ordered], axis=1)
            block_pos = jnp.concatenate(
                [(position - member[0]) * shard_len + offsets for member in ordered]
            )
            state_pair = attend_block(
                grouped, block_keys, block_values, query_pos, block_pos, state_pair
            )
            arrived = []
    numerator, denominator = state_pair
    attended = (numerator / jnp.transpose(denominator, (0, 3, 1, 2))[..., None]).astype(
        jnp.bfloat16
    )
    partial_value = jnp.dot(
        attended.reshape(seq_count * shard_len, query_width),
        out_weight,
        preferred_element_type=jnp.float32,
    )
    partial_value = partial_value.reshape(seq_count, shard_len, out_weight.shape[1])
    branch = lax.psum_scatter(partial_value, "tp", scatter_dimension=2, tiled=True)
    squares = lax.psum(jnp.sum(branch * branch, axis=-1), "tp")
    normed = branch * lax.rsqrt(squares / D + norm_eps)[..., None] * post_scale
    hidden_out = (residual.astype(jnp.float32) + normed).astype(jnp.bfloat16)
    block_rows = shard_len // seq_devices
    slot_span = WINDOW // shard_len
    live_rows = (query_pos[None, :] >= lengths[:, None] - WINDOW) & (
        query_pos[None, :] < lengths[:, None]
    )
    kept_keys = jnp.where(live_rows[..., None], key_rows, jnp.zeros_like(key_rows))
    kept_values = jnp.where(live_rows[..., None], value_rows, jnp.zeros_like(value_rows))
    devices = jnp.arange(seq_devices, dtype=jnp.int32)
    matches = owners[:, :, None] == devices[None, None, :]
    inverse = jnp.sum(
        jnp.where(matches, devices[None, :, None], jnp.zeros_like(devices)[None, :, None]), axis=1
    )
    outgoing_keys = jax.vmap(reorder_blocks)(
        kept_keys.reshape(seq_count, seq_devices, block_rows, kv_width), inverse
    )
    outgoing_values = jax.vmap(reorder_blocks)(
        kept_values.reshape(seq_count, seq_devices, block_rows, kv_width), inverse
    )
    incoming = (
        lax.all_to_all(outgoing_keys, "seq", split_axis=1, concat_axis=1, tiled=True),
        lax.all_to_all(outgoing_values, "seq", split_axis=1, concat_axis=1, tiled=True),
    )
    selector = (
        devices[None, :] % slot_span == jnp.arange(slot_span, dtype=jnp.int32)[:, None]
    ).astype(jnp.bfloat16)
    cache_keys = (
        jnp.einsum("md,sdbf->smbf", selector, incoming[0], preferred_element_type=jnp.float32)
        .astype(jnp.bfloat16)
        .reshape(seq_count, slot_span * block_rows, kv_width)
    )
    cache_values = (
        jnp.einsum("md,sdbf->smbf", selector, incoming[1], preferred_element_type=jnp.float32)
        .astype(jnp.bfloat16)
        .reshape(seq_count, slot_span * block_rows, kv_width)
    )
    return (hidden_out, cache_keys, cache_values)


def layer_kernel(
    n, q_hbm, k_hbm, v_hbm, res_hbm, scale_hbm, len_ref, own_hbm, w_ref,
    hid_hbm, ck_hbm, cv_hbm,
    hid_ref, ck_ref, cv_ref, q_ref, res_ref, scale_ref, own_ref, kstage, vstage, kgot, vgot,
    kbuf, vbuf, wbuf, acc, den, att, to_sib, to_x, to_sib2, from_sib, from_x, from_sib2,
    total, sq_out, sq_in,
    in_sem, send_sem, recv_sem, w_sem, rs_send, rs_recv, sq_send, sq_recv, cache_send, cache_recv, out_sem,
):
    nz = n // 2
    me = lax.axis_index("seq")
    t = lax.axis_index("tp")
    z, y = me // 2, me % 2
    x, c = t // 2, t % 2
    sib = x * 2 + (1 - c)
    across = (1 - x) * 2 + c
    diagonal = (1 - x) * 2 + (1 - c)
    shard = q_ref.shape[0]
    heads = q_ref.shape[1] // HD
    kv_width = k_hbm.shape[1]
    group = q_ref.shape[1] // kv_width
    block_rows = shard // n
    bufs = (kbuf, vbuf)
    loads = [
        pltpu.make_async_copy(src, dst, in_sem.at[i])
        for i, (src, dst) in enumerate(
            (
                (k_hbm, kbuf.at[me]), (v_hbm, vbuf.at[me]), (q_hbm, q_ref), (own_hbm, own_ref),
                (res_hbm, res_ref), (scale_hbm, scale_ref),
            )
        )
    ]
    for load in loads:
        load.start()

    def w_copy(f):
        return pltpu.make_async_copy(
            w_ref.at[:, pl.ds(f * res_ref.shape[1], res_ref.shape[1])], wbuf.at[f], w_sem.at[f]
        )

    partner = z * 2 + (1 - y)
    barrier = pltpu.get_barrier_semaphore()
    for peer in (sib, across, diagonal):
        pl.semaphore_signal(barrier, inc=1, device_id={"tp": peer}, device_id_type=MESH)
    for hop in range(1, n):
        pl.semaphore_signal(
            barrier, inc=1, device_id={"seq": lax.rem(me + hop, n)}, device_id_type=MESH
        )
    pl.semaphore_wait(barrier, n + 2)

    def routes(zo, yo, h):
        special = ((zo == 0) & (yo == 0)) if h == 1 else False
        line = (yo == y) | special
        crossing = (yo == y) & (zo + y <= z) & ((zo == z) | jnp.logical_not(special))
        origin = zo * 2 + yo
        plan = ((line & (zo <= z) & (z < nz - 1), me + 2), (crossing, partner))
        out = []
        for way, (go, to) in enumerate(plan):
            copy = pltpu.make_async_remote_copy(
                src_ref=bufs[h].at[origin],
                dst_ref=bufs[h].at[origin],
                send_sem=send_sem.at[origin, h, way],
                recv_sem=recv_sem.at[origin, h],
                device_id={"seq": to},
                device_id_type=MESH,
            )
            out.append((go, copy))
        return out

    def start(zo, yo, h):
        for go, copy in routes(zo, yo, h):
            pl.when(go)(copy.start)

    def handle(zo, yo, h):
        routes(zo, yo, h)[0][1].wait_recv()
        start(zo, yo, h)

    for h in (0, 1):
        loads[h].wait()
        start(z, y, h)
    for f in range(4):
        w_copy(f).start()
    loads[2].wait()
    loads[3].wait()

    def attend(keys, values, masked):
        for h in range(heads):
            cols = pl.ds((h // group) * HD, HD)
            s = lax.dot_general(
                q_ref[:, h * HD : (h + 1) * HD], keys[:, cols], (((1,), (1,)), ((), ())),
                preferred_element_type=jnp.float32,
            )
            w = jnp.exp2(jnp.tanh(s * (HD ** (-0.5) / soft_cap)) * (soft_cap * LOG2E))
            if masked:
                keep = lax.broadcasted_iota(jnp.int32, w.shape, 0) >= lax.broadcasted_iota(
                    jnp.int32, w.shape, 1
                )
                w = jnp.where(keep, w, 0.0)
            folded = w[:, :128]
            for i in range(1, w.shape[1] // 128):
                folded = folded + w[:, i * 128 : (i + 1) * 128]
            o = jnp.dot(w.astype(jnp.bfloat16), values[:, cols], preferred_element_type=jnp.float32)
            if masked:
                den[h] = folded
                acc[h] = o
            else:
                den[h] += folded
                acc[h] += o

    stages = ((kbuf, kstage, kgot), (vbuf, vstage, vgot))

    def cache_copy(h, to, slot):
        return pltpu.make_async_remote_copy(
            src_ref=stages[h][1].at[to], dst_ref=stages[h][2].at[slot],
            send_sem=cache_send.at[to, h], recv_sem=cache_recv.at[slot, h],
            device_id={"seq": to}, device_id_type=MESH,
        )

    def select(buf, origin, chosen):
        got = jnp.zeros(chosen.shape, jnp.float32)
        for b in range(n):
            rows = buf[origin, b * block_rows : (b + 1) * block_rows, :]
            got = jnp.where(chosen == b, rows.astype(jnp.float32), got)
        return got.astype(jnp.bfloat16)

    def owned(device):
        block = own_ref[0, 0] * 0
        for b in range(n):
            block = block + jnp.where(own_ref[0, b] == device, b, 0)
        return jnp.full((block_rows, kv_width), block, jnp.int32)

    def stage(to, carry):
        chosen = owned(to)
        for buf, staged, _ in stages:
            staged[to] = select(buf, me, chosen)
        return carry

    lax.fori_loop(0, me, stage, 0)
    attend(kbuf.at[me], vbuf.at[me], True)

    def post(to, carry):
        for h in (0, 1):
            cache_copy(h, to, me).start()
        return carry

    lax.fori_loop(0, me, post, 0)

    def phase(d, carry):
        e = d - 1
        for h in (0, 1):
            pl.when(z - d >= 0)(functools.partial(handle, z - d, y, h))
        for h in (1, 0):
            there = (z - e >= 0) & ((e > 0) | (y == 1))
            pl.when(there)(functools.partial(handle, z - e, 1 - y, h))

        def one(i, carry):
            zz = z - d + i
            origin = zz * 2 + jnp.where(i == 0, y, 1 - y)

            @pl.when((zz >= 0) & (origin < me))
            def _():
                attend(kbuf.at[origin], vbuf.at[origin], False)

            return carry

        lax.fori_loop(0, 2, one, 0)
        return carry

    lax.fori_loop(1, nz + 1, phase, 0)

    for h in range(heads):
        att[:, h * HD : (h + 1) * HD] = (
            acc[h] / jnp.sum(den[h], axis=-1, keepdims=True)
        ).astype(jnp.bfloat16)

    chunks = shard // ROWS

    def rs_copy(kind, r, src, dst, to):
        return pltpu.make_async_remote_copy(
            src_ref=src.at[r], dst_ref=dst.at[r], send_sem=rs_send.at[kind, r],
            recv_sem=rs_recv.at[kind, r], device_id={"tp": to}, device_id_type=MESH,
        )

    def sib_copy(r):
        return rs_copy(0, r, to_sib, from_sib, sib)

    def x_copy(r):
        return rs_copy(1, r, to_x, from_x, across)

    def sib2_copy(r):
        return rs_copy(2, r, to_sib2, from_sib2, sib)

    def part(f, r):
        rows = att[pl.ds(pl.multiple_of(r * ROWS, ROWS), ROWS), :]
        return jnp.dot(rows, wbuf[f], preferred_element_type=jnp.float32)

    for f in range(4):
        w_copy(f).wait()

    def first(r, carry):
        to_sib[r] = part(diagonal, r).astype(jnp.bfloat16)
        sib_copy(r).start()
        return carry

    def second(r, carry):
        mine = part(across, r)
        sib_copy(r).wait_recv()
        to_x[r] = (mine + from_sib[r].astype(jnp.float32)).astype(jnp.bfloat16)
        x_copy(r).start()
        return carry

    def third(r, carry):
        to_sib2[r] = part(sib, r).astype(jnp.bfloat16)
        sib2_copy(r).start()
        return carry

    def fourth(r, carry):
        total[r] = part(t, r)
        return carry

    for step in (first, second, third, fourth):
        lax.fori_loop(0, chunks, step, 0)

    chosen = owned(me)
    local_row = lax.broadcasted_iota(jnp.int32, chosen.shape, 0)
    bound = jnp.full(chosen.shape, len_ref[0], jnp.int32)

    def cache(origin, carry):
        pos = local_row + chosen * block_rows + origin * shard
        live = (pos < bound) & (pos >= bound - WINDOW)
        start_row = pl.multiple_of(origin * block_rows, block_rows)

        @pl.when(origin <= me)
        def _():
            spot = jnp.where(live, chosen, -1)
            for (buf, _, _), out in zip(stages, (ck_ref, cv_ref)):
                out[pl.ds(start_row, block_rows), :] = select(buf, origin, spot)

        @pl.when(origin > me)
        def _():
            for h, out in enumerate((ck_ref, cv_ref)):
                cache_copy(h, origin, origin).wait_recv()
                got = stages[h][2][origin].astype(jnp.float32)
                out[pl.ds(start_row, block_rows), :] = jnp.where(live, got, 0.0).astype(
                    jnp.bfloat16
                )

        return carry

    lax.fori_loop(0, n, cache, 0)
    rest = ck_ref.shape[0] - n * block_rows
    if rest:
        for out in (ck_ref, cv_ref):
            out[n * block_rows :, :] = jnp.zeros((rest, kv_width), jnp.bfloat16)
    outs = [
        pltpu.make_async_copy(src, dst, out_sem.at[i])
        for i, (src, dst) in enumerate(((ck_ref, ck_hbm), (cv_ref, cv_hbm), (hid_ref, hid_hbm)))
    ]
    outs[0].start()
    outs[1].start()

    for r in range(chunks):
        sib2_copy(r).wait_recv()
        x_copy(r).wait_recv()
        branch = total[r] + from_sib2[r].astype(jnp.float32) + from_x[r].astype(jnp.float32)
        total[r] = branch
        squared = branch * branch
        folded = squared[:, :128]
        for i in range(1, squared.shape[1] // 128):
            folded = folded + squared[:, i * 128 : (i + 1) * 128]
        line = jnp.sum(folded.T, axis=0, keepdims=True)
        sq_out[:, r * ROWS : (r + 1) * ROWS] = jnp.broadcast_to(line, (8, ROWS))

    def sq_copy(i, to, slot):
        return pltpu.make_async_remote_copy(
            src_ref=sq_out, dst_ref=sq_in.at[slot], send_sem=sq_send.at[i],
            recv_sem=sq_recv.at[slot], device_id={"tp": to}, device_id_type=MESH,
        )

    peers = (sib, across, diagonal)
    for i, peer in enumerate(peers):
        sq_copy(i, peer, t).start()
    squares = sq_out[...]
    for i, peer in enumerate(peers):
        sq_copy(i, peer, peer).wait_recv()
        squares = squares + sq_in[peer]
    loads[4].wait()
    loads[5].wait()
    factor = lax.rsqrt(squares / D + norm_eps)
    for r in range(chunks):
        line = jnp.broadcast_to(factor[:1, r * ROWS : (r + 1) * ROWS], (128, ROWS))
        spread = line.T
        for i in range(res_ref.shape[1] // 128):
            cols = slice(i * 128, (i + 1) * 128)
            rows = slice(r * ROWS, (r + 1) * ROWS)
            normed = total[r, :, cols] * spread * scale_ref[cols].reshape(1, 128)
            hid_ref[rows, cols] = (res_ref[rows, cols].astype(jnp.float32) + normed).astype(
                jnp.bfloat16
            )

    outs[2].start()
    for i, peer in enumerate(peers):
        sq_copy(i, peer, t).wait_send()
    for r in range(chunks):
        sib_copy(r).wait_send()
        x_copy(r).wait_send()
        sib2_copy(r).wait_send()

    def drain(origin, carry):
        for h in (0, 1):
            for go, copy in routes(origin // 2, origin % 2, h):
                pl.when(go)(copy.wait_send)
        return carry

    lax.fori_loop(0, me + 1, drain, 0)

    def settle(to, carry):
        for h in (0, 1):
            cache_copy(h, to, me).wait_send()
        return carry

    lax.fori_loop(0, me, settle, 0)
    for out in outs:
        out.wait()


def put_out(*refs):
    count = (len(refs) - 1) // 3
    sems = refs[-1]
    copies = [
        (
            pltpu.make_async_copy(refs[i], refs[2 * count + i], sems.at[0, i]),
            pltpu.make_async_copy(refs[2 * count + i], refs[count + i], sems.at[1, i]),
        )
        for i in range(count)
    ]
    for read, _ in copies:
        read.start()
    for read, write in copies:
        read.wait()
        write.start()
    for _, write in copies:
        write.wait()


def fused(n, queries, key_rows, value_rows, residual, out_weight, post_scale, lengths, owners):
    shard, q_width = queries.shape[1:]
    kv_width = key_rows.shape[2]
    width = residual.shape[2]
    heads = q_width // HD
    chunks = shard // ROWS
    cache_rows = WINDOW // n
    smem = pl.BlockSpec(memory_space=pltpu.SMEM)
    apart = pl.BlockSpec(memory_space=pl.ANY)
    owned_rows = pltpu.VMEM((n, shard // n, kv_width), jnp.bfloat16)
    half = pltpu.VMEM((chunks, ROWS, width), jnp.bfloat16)
    hidden, ck, cv = pl.pallas_call(
        functools.partial(layer_kernel, n),
        out_shape=(
            jax.ShapeDtypeStruct((shard, width), jnp.bfloat16),
            jax.ShapeDtypeStruct((cache_rows, kv_width), jnp.bfloat16),
            jax.ShapeDtypeStruct((cache_rows, kv_width), jnp.bfloat16),
        ),
        in_specs=[apart] * 5 + [smem] + [apart] * 2,
        out_specs=(apart,) * 3,
        scratch_shapes=[
            pltpu.VMEM((shard, width), jnp.bfloat16),
            pltpu.VMEM((cache_rows, kv_width), jnp.bfloat16),
            pltpu.VMEM((cache_rows, kv_width), jnp.bfloat16),
            pltpu.VMEM((shard, q_width), jnp.bfloat16),
            pltpu.VMEM((shard, width), jnp.bfloat16),
            pltpu.VMEM((width,), jnp.float32),
            pltpu.SMEM((1, n), jnp.int32),
            owned_rows, owned_rows, owned_rows, owned_rows,
            pltpu.VMEM((n, shard, kv_width), jnp.bfloat16),
            pltpu.VMEM((n, shard, kv_width), jnp.bfloat16),
            pltpu.VMEM((4, q_width, width), jnp.bfloat16),
            pltpu.VMEM((heads, shard, HD), jnp.float32),
            pltpu.VMEM((heads, shard, 128), jnp.float32),
            pltpu.VMEM((shard, q_width), jnp.bfloat16),
            half, half, half, half, half, half,
            pltpu.VMEM((chunks, ROWS, width), jnp.float32),
            pltpu.VMEM((8, shard), jnp.float32),
            pltpu.VMEM((4, 8, shard), jnp.float32),
            pltpu.SemaphoreType.DMA((6,)),
            pltpu.SemaphoreType.DMA((n, 2, 2)),
            pltpu.SemaphoreType.DMA((n, 2)),
            pltpu.SemaphoreType.DMA((4,)),
            pltpu.SemaphoreType.DMA((3, chunks)),
            pltpu.SemaphoreType.DMA((3, chunks)),
            pltpu.SemaphoreType.DMA((3,)),
            pltpu.SemaphoreType.DMA((4,)),
            pltpu.SemaphoreType.DMA((n, 2)),
            pltpu.SemaphoreType.DMA((n, 2)),
            pltpu.SemaphoreType.DMA((3,)),
        ],
        compiler_params=pltpu.CompilerParams(
            collective_id=0, has_side_effects=True, vmem_limit_bytes=60 * 1024 * 1024
        ),
    )(
        queries[0], key_rows[0], value_rows[0], residual[0], post_scale, lengths, owners,
        out_weight,
    )
    made = (hidden, ck, cv)
    hidden, ck, cv = pl.pallas_call(
        put_out,
        out_shape=tuple(jax.ShapeDtypeStruct(a.shape, a.dtype) for a in made),
        in_specs=[apart] * len(made),
        out_specs=(apart,) * len(made),
        scratch_shapes=[pltpu.VMEM(a.shape, a.dtype) for a in made]
        + [pltpu.SemaphoreType.DMA((2, len(made)))],
    )(*made)
    return hidden[None], ck[None], cv[None]


def solution(mesh):
    placed = (
        P(None, "seq", "tp"),
        P(None, "seq", "tp"),
        P(None, "seq", "tp"),
        P(None, "seq", "tp"),
        P("tp", None),
        P("tp"),
        P(),
        P(),
    )
    return jax.shard_map(
        local,
        mesh=mesh,
        in_specs=placed,
        out_specs=(P(None, "seq", "tp"), P(None, "seq", "tp"), P(None, "seq", "tp")),
        check_vma=False,
    )
```
